32 devices in a mesh: ctx: 8 (over z, y), heads: 4 (over x, core).
Axes of the slice: x: 2, y: 2, z: 4, core: 2. Of those that a mesh axis runs over, the one named last changes fastest.
Arguments:
- queries: bfloat16 [8192, 4096], P('ctx', 'heads'), may hold values from -8 to 8
- keys: bfloat16 [8192, 4096], P('ctx', 'heads'), may hold values from -8 to 8
- values: bfloat16 [8192, 4096], P('ctx', 'heads'), may hold values from -8 to 8
- gate_bias: float32 [32], P('heads'), may hold values from -2 to 2
- out_weight: bfloat16 [4096, 4096], P('heads'), may hold values from -0.09375 to 0.09375
Outputs:
- layer_out: bfloat16 [8192, 4096], P('ctx', 'heads')
The draws below stay inside these ranges and needn't reach their ends.
All inputs are finite; a program needn't handle non-finite values.
Results may differ from the reference program's by a relative error of at most 0.0051.
Values may be sent and summed in bfloat16 or wider, within the bound.
A program may use at most 128 MiB of HBM per device.

```python
import math
import jax
import jax.numpy as jnp
from jax import lax

D = 4096
HEADS = 32
HD = 128
SEG = 1024
TOKENS = 8192


class_count = 4


class_strength = 2.0


value_center = 1.6


def query_key_pair(key):
    folded = jax.random.fold_in(key, 11)
    seed_query = jax.random.fold_in(folded, 0)
    seed_key = jax.random.fold_in(folded, 1)
    seed_dirs = jax.random.fold_in(folded, 3)
    seed_qclass = jax.random.fold_in(folded, 4)
    seed_kclass = jax.random.fold_in(folded, 5)
    shape_full = (TOKENS, HEADS * HD)
    class_dirs = jax.random.rademacher(seed_dirs, (class_count, HEADS * HD)).astype(jnp.float32)
    query_class = jax.random.randint(seed_qclass, (TOKENS, HEADS), 0, class_count)
    key_class = jax.random.randint(seed_kclass, (TOKENS, HEADS), 0, class_count)
    query_dir = jnp.take_along_axis(class_dirs, jnp.repeat(query_class, HD, axis=1), axis=0)
    key_dir = jnp.take_along_axis(class_dirs, jnp.repeat(key_class, HD, axis=1), axis=0)
    query_noise = jnp.clip(jax.random.normal(seed_query, shape_full, jnp.float32), -4.0, 4.0)
    key_noise = jnp.clip(jax.random.normal(seed_key, shape_full, jnp.float32), -4.0, 4.0)
    query_draw = class_strength * query_dir + query_noise
    key_draw = class_strength * key_dir + key_noise
    return (jnp.clip(query_draw, -8.0, 8.0), jnp.clip(key_draw, -8.0, 8.0))


def draw_queries(key, part):
    return query_key_pair(key)[0].astype(jnp.bfloat16)


def draw_keys(key, part):
    return query_key_pair(key)[1].astype(jnp.bfloat16)


def draw_values(key, part):
    key_draw = query_key_pair(key)[1]
    folded = jax.random.fold_in(key, 23)
    seed_base, seed_offset, seed_mixing = jax.random.split(folded, 3)
    shape_full = (TOKENS, HEADS * HD)
    mixing = jax.random.normal(seed_mixing, (HEADS, HD, HD), jnp.float32) / math.sqrt(HD)
    centered = (jax.nn.elu(key_draw) + 1.0 - value_center).reshape(TOKENS, HEADS, HD)
    linked = jnp.einsum('thd,hde->the', centered, mixing, precision=lax.Precision.HIGHEST).reshape(shape_full)
    base_draw = jnp.clip(jax.random.normal(seed_base, shape_full, jnp.float32), -4.0, 4.0)
    offsets = jnp.clip(jax.random.normal(seed_offset, (TOKENS // SEG, HEADS * HD), jnp.float32), -3.0, 3.0)
    total = linked + 0.5 * base_draw + jnp.repeat(offsets, SEG, axis=0)
    return jnp.clip(total, -8.0, 8.0).astype(jnp.bfloat16)


def shard_levels(stream_key, extent, cuts, smallest, high):
    def one(dim, blocks):
        steps = jax.random.uniform(jax.random.fold_in(jax.random.fold_in(stream_key, 6), dim), (blocks,), jnp.float32, smallest / len(cuts), high / len(cuts))
        return jnp.repeat(jnp.exp(steps), extent[dim] // blocks).reshape((-1,) + (1,) * (len(extent) - dim - 1))

    loudness = one(*cuts[0])
    for cut in cuts[1:]:
        loudness = loudness * one(*cut)
    return loudness


def normal_values(own_key, extent, width, limit, cuts=(), kind=jnp.bfloat16):
    values = width * jax.random.normal(own_key, extent, jnp.float32)
    if cuts:
        values = values * shard_levels(own_key, extent, cuts, -0.22, 0.18)
    return jnp.clip(values, -limit, limit).astype(kind)


def setup_inputs(seed: int = 0) -> dict:
    splits = jax.random.split(jax.random.key(seed), 6)
    return {
        "queries": draw_queries(jax.random.fold_in(splits[5], 71), 0),
        "keys": draw_keys(jax.random.fold_in(splits[5], 71), 0),
        "values": draw_values(jax.random.fold_in(splits[5], 71), 0),
        "gate_bias": jnp.clip(jax.random.uniform(splits[3], (HEADS,), jnp.float32, -2.0, 2.0) * shard_levels(splits[3], (HEADS,), ((0, 4),), -0.4, 0.0), -2.0, 2.0),
        "out_weight": normal_values(splits[4], (HEADS * HD, D), (HEADS * HD) ** -0.5, 0.09375, ((0, 4),)),
    }


masked_score = -1e+30

def features(inputs):
    return jax.nn.elu(inputs) + 1.0

def head_attention(head_inputs):
    query_head, key_head, value_head = head_inputs
    seg_rows = query_head.shape[0]
    highest = lax.Precision.HIGHEST
    scores = jnp.dot(query_head, key_head.T, precision=highest) * (1.0 / math.sqrt(HD))
    positions = lax.iota(jnp.int32, seg_rows)
    allowed = positions[None, :] <= positions[:, None]
    scores = jnp.where(allowed, scores, masked_score)
    row_max = lax.optimization_barrier(jnp.max(scores, axis=-1, keepdims=True))
    weights = jnp.exp(scores - row_max)
    probabilities = (weights / lax.optimization_barrier(jnp.sum(weights, axis=-1, keepdims=True))).astype(jnp.bfloat16)
    return jnp.dot(probabilities.astype(query_head.dtype), value_head, precision=highest)

def local_attention(query_heads, key_heads, value_heads):
    per_head = lax.map(head_attention, (jnp.transpose(query_heads, (1, 0, 2)), jnp.transpose(key_heads, (1, 0, 2)), jnp.transpose(value_heads, (1, 0, 2))))
    return jnp.transpose(per_head, (1, 0, 2))

def reference(queries, keys, values, gate_bias, out_weight):
    segments = TOKENS // SEG
    query_blocks = queries.reshape(segments, SEG, HEADS, HD)
    key_blocks = keys.reshape(segments, SEG, HEADS, HD)
    value_blocks = values.reshape(segments, SEG, HEADS, HD)
    mix_gate = jax.nn.sigmoid(gate_bias.astype(jnp.float32))[None, :, None]
    highest = lax.Precision.HIGHEST

    def segment_step(state, inputs):
        memory, normalizer = state
        query_seg, key_seg, value_seg = inputs
        query_f = query_seg.astype(jnp.float32)
        key_f = key_seg.astype(jnp.float32)
        value_f = value_seg.astype(jnp.float32)
        feat_query = features(query_f)
        feat_key = features(key_f)
        local_out = local_attention(query_f, key_f, value_f)
        numer = jnp.einsum('thd,hde->the', feat_query, memory, precision=highest)
        denom = jnp.maximum(jnp.einsum('thd,hd->th', feat_query, normalizer, precision=highest), 1.0)
        retrieved = numer / denom[..., None]
        attended = (mix_gate * retrieved + (1.0 - mix_gate) * local_out).astype(jnp.bfloat16)
        memory = memory + jnp.einsum('thd,the->hde', feat_key, value_f, precision=highest)
        normalizer = normalizer + lax.optimization_barrier(jnp.sum(feat_key, axis=0))
        return ((memory, normalizer), attended)
    start_state = (jnp.zeros((HEADS, HD, HD), jnp.float32), jnp.zeros((HEADS, HD), jnp.float32))
    final_state, attended = lax.scan(segment_step, start_state, (query_blocks, key_blocks, value_blocks))
    attended = attended.reshape(TOKENS, HEADS * HD)
    return jnp.dot(attended, out_weight, preferred_element_type=jnp.float32).astype(jnp.bfloat16)
```

```python
import functools
import math

import jax
import jax.numpy as jnp
from jax import lax
from jax.experimental import pallas as pl
from jax.experimental.pallas import tpu as pltpu
from jax.sharding import PartitionSpec as P

HD = 128
MEM_ROWS = HD + 16
MESH = pl.DeviceIdType.MESH
masked_score = -1e30
F32 = jnp.float32
BF16 = jnp.bfloat16


def features(x):
    return jnp.where(x > 0.0, x + 1.0, jnp.exp(jnp.minimum(x, 0.0)))


def nt_dot(a, b):
    return lax.dot_general(a, b, (((1,), (1,)), ((), ())), preferred_element_type=F32)


def tn_dot(a, b):
    return lax.dot_general(a, b, (((0,), (0,)), ((), ())), preferred_element_type=F32)


def kernel(
    n_ctx, n_heads, block, tile,
    q_hbm, k_hbm, v_hbm, w_hbm, gate_ref, out_hbm,
    q_ref, k_ref, v_ref, w_ref, gates, delta, partner_delta, pair_sum, slots, prior_sum, prior,
    mixed, own_rows, partner_rows, cross_out, cross_in, out_stage,
    in_sem, w_sem, w_send, w_recv, pd_send, pd_recv, ps_send, ps_recv,
    rows_send, rows_recv, cross_send, cross_recv, out_sem,
):
    seg = lax.axis_index("ctx")
    col = lax.axis_index("heads")
    core = col % 2
    chip = col // 2
    other_col = col + 1 - 2 * core
    odd = seg % 2
    pair = seg // 2
    other_seg = seg + 1 - 2 * odd
    n_pairs = n_ctx // 2
    n_chips = n_heads // 2
    tokens, width = q_ref.shape
    heads = width // HD
    n_blocks = tokens // block

    loads = [
        pltpu.make_async_copy(src, dst, in_sem.at[i])
        for i, (src, dst) in enumerate(((k_hbm, k_ref), (v_hbm, v_ref), (q_hbm, q_ref)))
    ]
    for load in loads:
        load.start()

    def w_cols(target_chip, target_core):
        first = pl.multiple_of((target_chip * 2 + target_core) * width, width)
        return w_hbm.at[:, pl.ds(first, width)]

    w_loads = [
        pltpu.make_async_copy(w_cols(t, core), w_ref.at[0, t], w_sem.at[t]) for t in range(n_chips)
    ]
    for load in w_loads:
        load.start()

    barrier = pltpu.get_barrier_semaphore()
    peers = [(seg, other_col), (other_seg, col)]
    for o in range(1, n_chips):
        peers.append((seg, lax.rem(chip + o, n_chips) * 2 + core))
    for o in range(1, n_pairs):
        peers.append((lax.rem(pair + o, n_pairs) * 2 + odd, col))
    for peer in peers:
        pl.semaphore_signal(barrier, inc=1, device_id=peer, device_id_type=MESH)
    pl.semaphore_wait(barrier, len(peers))

    def remote(src, dst, send, recv, peer):
        return pltpu.make_async_remote_copy(
            src_ref=src, dst_ref=dst, send_sem=send, recv_sem=recv,
            device_id=peer, device_id_type=MESH,
        )

    def w_copy(t):
        return remote(
            w_cols(t, 1 - core), w_ref.at[1, t], w_send.at[t], w_recv.at[t], (seg, other_col)
        )

    def delta_copy(h):
        return remote(
            delta.at[h], partner_delta.at[h], pd_send.at[h], pd_recv.at[h], (other_seg, col)
        )

    def pair_copy(o, h):
        peer = (lax.rem(pair + o, n_pairs) * 2 + odd, col)
        return remote(
            pair_sum.at[h], slots.at[o - 1, h], ps_send.at[o - 1, h], ps_recv.at[o - 1, h], peer
        )

    def rows_copy(b):
        rows = pl.ds(b * block, block)
        return remote(
            own_rows.at[rows], partner_rows.at[rows], rows_send.at[b], rows_recv.at[b],
            (seg, other_col),
        )

    def cross_copy(o, b):
        rows = pl.ds(b * block, block)
        peer = (seg, lax.rem(chip + o, n_chips) * 2 + core)
        return remote(
            cross_out.at[o - 1, rows], cross_in.at[o - 1, rows],
            cross_send.at[o - 1, b], cross_recv.at[o - 1, b], peer,
        )

    def head_cols(h):
        return pl.ds(pl.multiple_of(h * HD, HD), HD)

    for t in range(n_chips):
        w_copy(t).start()

    gate_values = 1.0 / (1.0 + jnp.exp(-gate_ref[...]))
    for h in range(heads):
        gates[0:1, h * HD : (h + 1) * HD] = jnp.broadcast_to(gate_values[0:1, h : h + 1], (1, HD))

    loads[0].wait()
    loads[1].wait()

    @pl.loop(0, heads)
    def _(h):
        feat = features(k_ref[:, head_cols(h)].astype(F32))
        memory = tn_dot(v_ref[:, head_cols(h)], feat.astype(BF16))
        normal = jnp.sum(feat, axis=0, keepdims=True)
        delta[h, 0:HD, :] = memory.astype(BF16)
        delta[h, HD:MEM_ROWS, :] = jnp.broadcast_to(normal, (MEM_ROWS - HD, HD)).astype(BF16)
        delta_copy(h).start()

    loads[2].wait()

    scale = math.log2(math.e) / math.sqrt(HD)

    def attend(h):
        cols = head_cols(h)
        gate = 1.0 - gates[0:1, cols]
        ones = jnp.ones((tokens, HD), BF16)
        value_ext = jnp.concatenate([v_ref[:, cols], ones], axis=1)
        keys = k_ref[:, cols]
        row_ids = lax.broadcasted_iota(jnp.int32, (block, block), 0)
        col_ids = lax.broadcasted_iota(jnp.int32, (block, block), 1)
        allowed = col_ids <= row_ids
        for b in range(n_blocks):
            first = b * block
            query = q_ref[first : first + block, cols]
            diag = nt_dot(query, keys[first : first + block])
            diag = jnp.where(allowed, diag * scale, masked_score)
            top = jnp.max(diag, axis=1, keepdims=True)
            if b:
                past = nt_dot(query, keys[:first]) * scale
                top = jnp.maximum(top, jnp.max(past, axis=1, keepdims=True))
            total = jnp.dot(
                jnp.exp2(diag - top).astype(BF16), value_ext[first : first + block],
                preferred_element_type=F32,
            )
            if b:
                total = total + jnp.dot(
                    jnp.exp2(past - top).astype(BF16), value_ext[:first],
                    preferred_element_type=F32,
                )
            mixed[first : first + block, cols] = gate * (total[:, :HD] / total[:, HD:])

    group = 2 if heads % 2 == 0 else 1
    rounds = heads // group
    chunk = min(2 * group, heads)
    chunks = pl.cdiv(heads, chunk)

    @pl.loop(0, rounds)
    def _(i):
        for g in range(group):
            attend(i * group + g)

        @pl.when(i < chunks)
        def _():
            @pl.loop(0, chunk)
            def _(c):
                h = i * chunk + c
                delta_copy(h).wait_recv()
                pair_sum[h] = (delta[h].astype(F32) + partner_delta[h].astype(F32)).astype(BF16)
                for o in range(1, n_pairs):
                    @pl.when(pair + o < n_pairs)
                    def _():
                        pair_copy(o, h).start()

    odd_mask = jnp.where(odd == 1, 1.0, 0.0).astype(F32)

    @pl.loop(0, heads)
    def _(h):
        prior_sum[h] = partner_delta[h].astype(F32) * odd_mask

    for o in range(1, n_pairs):
        @pl.when(pair >= o)
        def _():
            @pl.loop(0, heads)
            def _(h):
                pair_copy(o, h).wait_recv()
                prior_sum[h] += slots[o - 1, h].astype(F32)

    @pl.loop(0, heads)
    def _(h):
        prior[h, 0:HD, :] = prior_sum[h, 0:HD, :].astype(BF16)
        prior[h, HD : 2 * HD, :] = jnp.broadcast_to(
            prior_sum[h, HD : HD + 1, :], (HD, HD)
        ).astype(BF16)

    for t in range(n_chips):
        w_loads[t].wait()
        w_copy(t).wait_recv()

    def finish(b):
        rows = pl.ds(b * block, block)

        @pl.loop(0, heads // group)
        def _(i):
            for g in range(group):
                cols = head_cols(i * group + g)
                feat = features(q_ref[rows, cols].astype(F32)).astype(BF16)
                both = nt_dot(feat, prior[i * group + g])
                retrieved = both[:, :HD] / jnp.maximum(both[:, HD:], 1.0)
                own_rows[rows, cols] = (gates[0:1, cols] * retrieved + mixed[rows, cols]).astype(BF16)

        rows_copy(b).start()

    def product(b, target, t):
        rows = pl.ds(b * block, block)
        cols = pl.ds(pl.multiple_of(t * tile, tile), tile)
        return jnp.dot(
            own_rows[rows], w_ref[0, target, :, cols], preferred_element_type=F32
        ) + jnp.dot(
            partner_rows[rows], w_ref[1, target, :, cols], preferred_element_type=F32
        )

    def cross(b):
        rows_copy(b).wait_recv()
        for o in range(1, n_chips):
            target = lax.rem(chip + o, n_chips)

            @pl.loop(0, width // tile)
            def _(t):
                cols = pl.ds(pl.multiple_of(t * tile, tile), tile)
                cross_out[o - 1, pl.ds(b * block, block), cols] = product(b, target, t).astype(BF16)

            cross_copy(o, b).start()

    finish(0)
    for b in range(n_blocks):
        if b + 1 < n_blocks:
            finish(b + 1)
        cross(b)

    @pl.loop(0, n_blocks)
    def _(b):
        @pl.loop(0, width // tile)
        def _(t):
            cols = pl.ds(pl.multiple_of(t * tile, tile), tile)
            mixed[pl.ds(b * block, block), cols] = product(b, chip, t)

    def out_copy(b):
        rows = pl.ds(b * block, block)
        return pltpu.make_async_copy(out_stage.at[rows], out_hbm.at[rows], out_sem.at[b])

    for b in range(n_blocks):
        rows = pl.ds(b * block, block)
        total = mixed[rows]
        for o in range(1, n_chips):
            cross_copy(o, b).wait_recv()
            total = total + cross_in[o - 1, rows].astype(F32)
        out_stage[rows] = total.astype(BF16)
        out_copy(b).start()

    for t in range(n_chips):
        w_copy(t).wait_send()

    @pl.loop(0, heads)
    def _(h):
        delta_copy(h).wait_send()
        for o in range(1, n_pairs):
            @pl.when(pair + o < n_pairs)
            def _():
                pair_copy(o, h).wait_send()

    for b in range(n_blocks):
        rows_copy(b).wait_send()
        for o in range(1, n_chips):
            cross_copy(o, b).wait_send()
        out_copy(b).wait()


def local(n_ctx, n_heads, queries, keys, values, gate_bias, out_weight):
    tokens, width = queries.shape
    heads = gate_bias.shape[0]
    block = min(256, tokens)
    tile = min(512, width)
    n_blocks = tokens // block
    n_pairs = n_ctx // 2
    n_chips = n_heads // 2
    dma = pltpu.SemaphoreType.DMA
    far_pairs = max(n_pairs - 1, 1)
    far_chips = max(n_chips - 1, 1)
    hbm = pl.BlockSpec(memory_space=pl.ANY)
    memories = (heads, MEM_ROWS, HD)
    return pl.pallas_call(
        functools.partial(kernel, n_ctx, n_heads, block, tile),
        out_shape=jax.ShapeDtypeStruct((tokens, width), BF16),
        in_specs=[hbm, hbm, hbm, hbm, pl.BlockSpec(memory_space=pltpu.VMEM)],
        out_specs=hbm,
        scratch_shapes=[
            pltpu.VMEM((tokens, width), BF16),
            pltpu.VMEM((tokens, width), BF16),
            pltpu.VMEM((tokens, width), BF16),
            pltpu.VMEM((2, n_chips, width, width), BF16),
            pltpu.VMEM((1, width), F32),
            pltpu.VMEM(memories, BF16),
            pltpu.VMEM(memories, BF16),
            pltpu.VMEM(memories, BF16),
            pltpu.VMEM((far_pairs,) + memories, BF16),
            pltpu.VMEM(memories, F32),
            pltpu.VMEM((heads, 2 * HD, HD), BF16),
            pltpu.VMEM((tokens, width), F32),
            pltpu.VMEM((tokens, width), BF16),
            pltpu.VMEM((tokens, width), BF16),
            pltpu.VMEM((far_chips, tokens, width), BF16),
            pltpu.VMEM((far_chips, tokens, width), BF16),
            pltpu.VMEM((tokens, width), BF16),
            dma((3,)),
            dma((n_chips,)),
            dma((n_chips,)),
            dma((n_chips,)),
            dma((heads,)),
            dma((heads,)),
            dma((far_pairs, heads)),
            dma((far_pairs, heads)),
            dma((n_blocks,)),
            dma((n_blocks,)),
            dma((far_chips, n_blocks)),
            dma((far_chips, n_blocks)),
            dma((n_blocks,)),
        ],
        compiler_params=pltpu.CompilerParams(
            collective_id=0, has_side_effects=True, vmem_limit_bytes=60 * 1024 * 1024
        ),
    )(queries, keys, values, out_weight, gate_bias.reshape(1, heads))


def solution(mesh):
    return jax.shard_map(
        functools.partial(local, mesh.shape["ctx"], mesh.shape["heads"]),
        mesh=mesh,
        in_specs=(
            P("ctx", "heads"),
            P("ctx", "heads"),
            P("ctx", "heads"),
            P("heads"),
            P("heads", None),
        ),
        out_specs=P("ctx", "heads"),
        check_vma=False,
    )
```

```python
import functools
import math

import jax
import jax.numpy as jnp
from jax import lax
from jax.experimental import pallas as pl
from jax.experimental.pallas import tpu as pltpu
from jax.sharding import PartitionSpec as P

HD = 128
MEM_ROWS = HD + 16
MESH = pl.DeviceIdType.MESH
masked_score = -1e30
F32 = jnp.float32
BF16 = jnp.bfloat16


def features(x):
    return jnp.where(x > 0.0, x + 1.0, jnp.exp(jnp.minimum(x, 0.0)))


def nt_dot(a, b):
    return lax.dot_general(a, b, (((1,), (1,)), ((), ())), preferred_element_type=F32)


def tn_dot(a, b):
    return lax.dot_general(a, b, (((0,), (0,)), ((), ())), preferred_element_type=F32)


def kernel(
    n_ctx, n_heads, block, blocks, tile,
    q_hbm, k_hbm, v_hbm, w_hbm, gate_ref, out_ref,
    q_ref, k_ref, v_ref, w_ref, gates, delta, partner_delta, running, arrived, prior,
    mixed, own_rows, partner_rows, cross_out, cross_in,
    in_sem, w_sem, w_send, w_recv, pd_send, pd_recv, run_send, run_recv,
    rows_send, rows_recv, cross_send, cross_recv,
):
    seg = lax.axis_index("ctx")
    col = lax.axis_index("heads")
    core = col % 2
    chip = col // 2
    other_col = col + 1 - 2 * core
    odd = seg % 2
    pair = seg // 2
    other_seg = seg + 1 - 2 * odd
    n_pairs = n_ctx // 2
    n_chips = n_heads // 2
    tokens, width = q_ref.shape
    heads = width // HD
    n_blocks = len(blocks)

    loads = [
        pltpu.make_async_copy(src, dst, in_sem.at[i])
        for i, (src, dst) in enumerate(((k_hbm, k_ref), (v_hbm, v_ref), (q_hbm, q_ref)))
    ]
    loads[0].start()
    loads[1].start()

    def w_cols(target_chip, target_core):
        first = pl.multiple_of((target_chip * 2 + target_core) * width, width)
        return w_hbm.at[:, pl.ds(first, width)]

    w_loads = [
        pltpu.make_async_copy(w_cols(t, core), w_ref.at[0, t], w_sem.at[t]) for t in range(n_chips)
    ]

    barrier = pltpu.get_barrier_semaphore()
    peers = [(seg, other_col), (other_seg, col)]
    for o in range(1, n_chips):
        peers.append((seg, lax.rem(chip + o, n_chips) * 2 + core))
    for o in (1, n_pairs - 1):
        peers.append((lax.rem(pair + o, n_pairs) * 2 + odd, col))
    for peer in peers:
        pl.semaphore_signal(barrier, inc=1, device_id=peer, device_id_type=MESH)
    pl.semaphore_wait(barrier, len(peers))

    def remote(src, dst, send, recv, peer):
        return pltpu.make_async_remote_copy(
            src_ref=src, dst_ref=dst, send_sem=send, recv_sem=recv,
            device_id=peer, device_id_type=MESH,
        )

    def w_copy(t):
        return remote(
            w_cols(t, 1 - core), w_ref.at[1, t], w_send.at[t], w_recv.at[t], (seg, other_col)
        )

    def delta_copy(h):
        return remote(
            delta.at[h], partner_delta.at[h], pd_send.at[h], pd_recv.at[h], (other_seg, col)
        )

    def run_copy(h):
        peer = (lax.rem(pair + 1, n_pairs) * 2 + odd, col)
        return remote(running.at[h], arrived.at[h], run_send.at[h], run_recv.at[h], peer)

    def rows_copy(b):
        rows = pl.ds(*blocks[b])
        return remote(
            own_rows.at[rows], partner_rows.at[rows], rows_send.at[b], rows_recv.at[b],
            (seg, other_col),
        )

    def cross_copy(o, b):
        rows = pl.ds(*blocks[b])
        peer = (seg, lax.rem(chip + o, n_chips) * 2 + core)
        return remote(
            cross_out.at[o - 1, rows], cross_in.at[o - 1, rows],
            cross_send.at[o - 1, b], cross_recv.at[o - 1, b], peer,
        )

    def head_cols(h):
        return pl.ds(pl.multiple_of(h * HD, HD), HD)

    gate_values = 1.0 / (1.0 + jnp.exp(-gate_ref[...]))
    for h in range(heads):
        gates[0:1, h * HD : (h + 1) * HD] = jnp.broadcast_to(gate_values[0:1, h : h + 1], (1, HD))

    loads[0].wait()
    loads[1].wait()
    loads[2].start()
    for t in range(n_chips):
        w_copy(t).start()
        w_loads[t].start()

    @pl.loop(0, heads)
    def _(h):
        feat = features(k_ref[:, head_cols(h)].astype(F32))
        memory = tn_dot(v_ref[:, head_cols(h)], feat.astype(BF16))
        normal = jnp.sum(feat, axis=0, keepdims=True)
        delta[h, 0:HD, :] = memory.astype(BF16)
        delta[h, HD:MEM_ROWS, :] = jnp.broadcast_to(normal, (MEM_ROWS - HD, HD)).astype(BF16)
        delta_copy(h).start()

    loads[2].wait()

    scale = math.log2(math.e) / math.sqrt(HD)

    def attend(h):
        cols = head_cols(h)
        gate = 1.0 - gates[0:1, cols]
        ones = jnp.ones((tokens, HD), BF16)
        value_ext = jnp.concatenate([v_ref[:, cols], ones], axis=1)
        keys = k_ref[:, cols]
        row_ids = lax.broadcasted_iota(jnp.int32, (block, block), 0)
        col_ids = lax.broadcasted_iota(jnp.int32, (block, block), 1)
        allowed = col_ids <= row_ids
        for b in range(tokens // block):
            first = b * block
            query = q_ref[first : first + block, cols]
            diag = nt_dot(query, keys[first : first + block])
            diag = jnp.where(allowed, diag * scale, masked_score)
            top = jnp.max(diag, axis=1, keepdims=True)
            if b:
                past = nt_dot(query, keys[:first]) * scale
                top = jnp.maximum(top, jnp.max(past, axis=1, keepdims=True))
            total = jnp.dot(
                jnp.exp2(diag - top).astype(BF16), value_ext[first : first + block],
                preferred_element_type=F32,
            )
            if b:
                total = total + jnp.dot(
                    jnp.exp2(past - top).astype(BF16), value_ext[:first],
                    preferred_element_type=F32,
                )
            mixed[first : first + block, cols] = gate * (total[:, :HD] / total[:, HD:])

    odd_mask = jnp.where(odd == 1, 1.0, 0.0).astype(F32)

    def finish_head(b, h):
        rows = pl.ds(*blocks[b])
        cols = head_cols(h)
        feat = features(q_ref[rows, cols].astype(F32)).astype(BF16)
        both = nt_dot(feat, prior[h])
        retrieved = both[:, :HD] / jnp.maximum(both[:, HD:], 1.0)
        own_rows[rows, cols] = (gates[0:1, cols] * retrieved + mixed[rows, cols]).astype(BF16)

    def relay(h):
        delta_copy(h).wait_recv()
        theirs = partner_delta[h].astype(F32)

        @pl.when(pair == 0)
        def _():
            arrived[h] = jnp.zeros((MEM_ROWS, HD), BF16)

        @pl.when(pair > 0)
        def _():
            run_copy(h).wait_recv()

        before = arrived[h].astype(F32)

        @pl.when(pair + 1 < n_pairs)
        def _():
            running[h] = (before + (delta[h].astype(F32) + theirs)).astype(BF16)
            run_copy(h).start()

        mine = before + theirs * odd_mask
        prior[h, 0:HD, :] = mine[0:HD].astype(BF16)
        prior[h, HD : 2 * HD, :] = jnp.broadcast_to(mine[HD : HD + 1], (HD, HD)).astype(BF16)

    lag = jnp.minimum(1 + 2 * pair, heads)

    @pl.loop(0, 2 * heads)
    def _(i):
        @pl.when(i < heads)
        def _():
            attend(i)

        h = i - lag

        @pl.when((h >= 0) & (h < heads))
        def _():
            relay(h)

    for t in range(n_chips):
        w_loads[t].wait()
        w_copy(t).wait_recv()

    group = 2 if heads % 2 == 0 else 1

    def finish(b):
        @pl.loop(0, heads // group)
        def _(i):
            for g in range(group):
                finish_head(b, i * group + g)

        rows_copy(b).start()

    def product(b, target, t):
        rows = pl.ds(*blocks[b])
        cols = pl.ds(pl.multiple_of(t * tile, tile), tile)
        return jnp.dot(
            own_rows[rows], w_ref[0, target, :, cols], preferred_element_type=F32
        ) + jnp.dot(
            partner_rows[rows], w_ref[1, target, :, cols], preferred_element_type=F32
        )

    def cross(b):
        rows_copy(b).wait_recv()
        for o in range(1, n_chips):
            target = lax.rem(chip + o, n_chips)

            @pl.loop(0, width // tile)
            def _(t):
                cols = pl.ds(pl.multiple_of(t * tile, tile), tile)
                cross_out[o - 1, pl.ds(*blocks[b]), cols] = product(b, target, t).astype(BF16)

            cross_copy(o, b).start()

    finish(0)
    for b in range(n_blocks):
        if b + 1 < n_blocks:
            finish(b + 1)
        cross(b)

    for b in range(n_blocks):
        @pl.loop(0, width // tile)
        def _(t):
            cols = pl.ds(pl.multiple_of(t * tile, tile), tile)
            mixed[pl.ds(*blocks[b]), cols] = product(b, chip, t)

    for b in range(n_blocks):
        rows = pl.ds(*blocks[b])
        total = mixed[rows]
        for o in range(1, n_chips):
            cross_copy(o, b).wait_recv()
            total = total + cross_in[o - 1, rows].astype(F32)
        out_ref[rows] = total.astype(BF16)

    for t in range(n_chips):
        w_copy(t).wait_send()

    @pl.loop(0, heads)
    def _(h):
        delta_copy(h).wait_send()

        @pl.when(pair + 1 < n_pairs)
        def _():
            run_copy(h).wait_send()

    for b in range(n_blocks):
        rows_copy(b).wait_send()
        for o in range(1, n_chips):
            cross_copy(o, b).wait_send()


def local(n_ctx, n_heads, queries, keys, values, gate_bias, out_weight):
    tokens, width = queries.shape
    heads = gate_bias.shape[0]
    block = min(256, tokens)
    tile = min(512, width)
    sizes = [block] * (tokens // block)
    if len(sizes) > 1 and block % 32 == 0:
        sizes = [block // 2] + [block] * (len(sizes) - 1) + [block // 2]
    blocks = [(sum(sizes[:b]), size) for b, size in enumerate(sizes)]
    n_blocks = len(blocks)
    n_chips = n_heads // 2
    dma = pltpu.SemaphoreType.DMA
    far_chips = max(n_chips - 1, 1)
    hbm = pl.BlockSpec(memory_space=pltpu.HBM)
    memories = (heads, MEM_ROWS, HD)
    return pl.pallas_call(
        functools.partial(kernel, n_ctx, n_heads, block, blocks, tile),
        out_shape=jax.ShapeDtypeStruct((tokens, width), BF16),
        in_specs=[hbm, hbm, hbm, hbm, pl.BlockSpec(memory_space=pltpu.VMEM)],
        out_specs=pl.BlockSpec(memory_space=pltpu.VMEM),
        scratch_shapes=[
            pltpu.VMEM((tokens, width), BF16),
            pltpu.VMEM((tokens, width), BF16),
            pltpu.VMEM((tokens, width), BF16),
            pltpu.VMEM((2, n_chips, width, width), BF16),
            pltpu.VMEM((1, width), F32),
            pltpu.VMEM(memories, BF16),
            pltpu.VMEM(memories, BF16),
            pltpu.VMEM(memories, BF16),
            pltpu.VMEM(memories, BF16),
            pltpu.VMEM((heads, 2 * HD, HD), BF16),
            pltpu.VMEM((tokens, width), F32),
            pltpu.VMEM((tokens, width), BF16),
            pltpu.VMEM((tokens, width), BF16),
            pltpu.VMEM((far_chips, tokens, width), BF16),
            pltpu.VMEM((far_chips, tokens, width), BF16),
            dma((3,)),
            dma((n_chips,)),
            dma((n_chips,)),
            dma((n_chips,)),
            dma((heads,)),
            dma((heads,)),
            dma((heads,)),
            dma((heads,)),
            dma((n_blocks,)),
            dma((n_blocks,)),
            dma((far_chips, n_blocks)),
            dma((far_chips, n_blocks)),
        ],
        compiler_params=pltpu.CompilerParams(
            collective_id=0, has_side_effects=True, vmem_limit_bytes=63_000 * 1024
        ),
    )(queries, keys, values, out_weight, gate_bias.reshape(1, heads))


def solution(mesh):
    return jax.shard_map(
        functools.partial(local, mesh.shape["ctx"], mesh.shape["heads"]),
        mesh=mesh,
        in_specs=(
            P("ctx", "heads"),
            P("ctx", "heads"),
            P("ctx", "heads"),
            P("heads"),
            P("heads", None),
        ),
        out_specs=P("ctx", "heads"),
        check_vma=False,
    )
```
